32 devices in a mesh: dp: 4 (over y, x), col: 8 (over z, core).
Axes of the slice: x: 2, y: 2, z: 4, core: 2. Of those that a mesh axis runs over, the one named last changes fastest.
Arguments:
- tokens: bfloat16 [1536, 2304], P('dp', 'col'), may hold values from -6 to 6
- cotangent: bfloat16 [1536, 2304], P('dp', 'col'), may hold values from -6 to 6
- prefix: int32 [12], P('dp'), may hold values from 0 to 3
- gate_weight: bfloat16 [2304, 36864], P(None, 'col'), may hold values from -0.125 to 0.125
- up_weight: bfloat16 [2304, 36864], P(None, 'col'), may hold values from -0.125 to 0.125
- down_weight: bfloat16 [36864, 2304], P('col'), may hold values from -0.0625 to 0.0625
Outputs:
- output: bfloat16 [1536, 2304], P('dp', 'col')
- input_grad: bfloat16 [1536, 2304], P('dp', 'col')
- grad_gate: bfloat16 [2304, 36864], P('dp', 'col')
- grad_up: bfloat16 [2304, 36864], P('dp', 'col')
- grad_down: bfloat16 [36864, 2304], P('col', 'dp')
The draws below stay inside these ranges and needn't reach their ends.
All inputs are finite; a program needn't handle non-finite values.
Results may differ from the reference program's by a relative error of at most 0.017.
Values may be sent and summed in bfloat16 or wider, within the bound.
No kernel may reach another device: no remote copies, remote signals or barrier semaphores. Data moves between devices by JAX's collectives and lax.ppermute only.
A program may use at most 256 MiB of HBM per device.

```python
import jax
import jax.numpy as jnp

D = 2304
FF = 36864
BLOCK = 128
TOK_DEV = 384
TOKENS = 1536
BLOCKS = 12
N_DP = 4


def set_ends(result, stream_key, smallest, high):
    place = [jax.random.randint(jax.random.fold_in(stream_key, axis), (), 0, length) for axis, length in enumerate(result.shape)]
    main_axis = result.shape.index(max(result.shape))
    neighbour = place[:main_axis] + [(place[main_axis] + 1) % result.shape[main_axis]] + place[main_axis + 1:]
    return result.at[tuple(place)].set(smallest).at[tuple(neighbour)].set(high)


def levels(own_key, extent, pieces, smallest, largest):
    gain = 1.0
    for axis_at, parts in pieces:
        steps = jax.random.uniform(jax.random.fold_in(jax.random.fold_in(own_key, 6), axis_at), (parts,), jnp.float32, smallest / len(pieces), largest / len(pieces))
        gain = gain * jnp.repeat(jnp.exp(steps), extent[axis_at] // parts).reshape((-1,) + (1,) * (len(extent) - 1 - axis_at))
    return gain


def centred(own_key, dims, scale, reach, cuts=(), held_as=jnp.bfloat16):
    result = jax.random.normal(own_key, dims, jnp.float32) * scale
    if len(cuts) > 0:
        result = levels(own_key, dims, cuts, -0.22, 0.18) * result
    return jnp.clip(result, min=-reach, max=reach).astype(held_as)


def setup_inputs(seed: int = 0) -> dict:
    streams_of = jax.random.split(jax.random.key(seed), 7)
    tokens = centred(streams_of[0], (TOKENS, D), 1.0, 6.0, ((0, 4), (1, 8)))
    cotangent = centred(streams_of[1], (TOKENS, D), 1.0, 6.0, ((0, 4), (1, 8)))
    prefix = set_ends(jax.random.randint(streams_of[2], (BLOCKS,), 0, 4), jax.random.fold_in(streams_of[2], 1), 0, 3).astype(jnp.int32)
    gate_weight = centred(streams_of[3], (D, FF), D ** -0.5, 0.125, ((1, 8),))
    up_weight = centred(streams_of[4], (D, FF), D ** -0.5, 0.125, ((1, 8),))
    down_weight = centred(streams_of[5], (FF, D), (FF // 4) ** -0.5, 0.0625, ((0, 8),))
    return {"tokens": tokens, "cotangent": cotangent, "prefix": prefix, "gate_weight": gate_weight, "up_weight": up_weight, "down_weight": down_weight}


def gelu_pair(value):
    scale = 0.7978845608028654
    inner = jnp.tanh(scale * (value + 0.044715 * value * value * value))
    act = 0.5 * value * (1.0 + inner)
    slope = 0.5 * (1.0 + inner) + 0.5 * value * (1.0 - inner * inner) * scale * (1.0 + 3.0 * 0.044715 * value * value)
    return act, slope


def matmul(left, right):
    return jnp.dot(left.astype(jnp.float32), right.astype(jnp.float32))


def reference(tokens, cotangent, prefix, gate_weight, up_weight, down_weight):
    widths = jnp.left_shift(jnp.int32(FF // 8), prefix.astype(jnp.int32))
    per_token = jnp.repeat(widths, BLOCK, total_repeat_length=TOKENS)
    columns = jnp.arange(FF, dtype=jnp.int32)
    mask = (columns[None, :] < per_token[:, None]).astype(jnp.float32)
    gate = matmul(tokens, gate_weight)
    up = matmul(tokens, up_weight)
    act, slope = gelu_pair(gate)
    hidden = (mask * act * up).astype(jnp.bfloat16)
    output = matmul(hidden, down_weight).astype(jnp.bfloat16)
    back = matmul(cotangent, down_weight.T)
    dgate = (mask * back * up * slope).astype(jnp.bfloat16)
    dup = (mask * back * act).astype(jnp.bfloat16)
    input_grad = (matmul(dgate, gate_weight.T) + matmul(dup, up_weight.T)).astype(jnp.bfloat16)
    sum_gate = jnp.zeros((D, FF), jnp.float32)
    sum_up = jnp.zeros((D, FF), jnp.float32)
    sum_down = jnp.zeros((FF, D), jnp.float32)
    for group in range(N_DP):
        first = group * TOK_DEV
        last = first + TOK_DEV
        sum_gate = sum_gate + matmul(tokens[first:last].T, dgate[first:last]).astype(jnp.bfloat16).astype(jnp.float32)
        sum_up = sum_up + matmul(tokens[first:last].T, dup[first:last]).astype(jnp.bfloat16).astype(jnp.float32)
        sum_down = sum_down + matmul(hidden[first:last].T, cotangent[first:last]).astype(jnp.bfloat16).astype(jnp.float32)
    return (output, input_grad, sum_gate.astype(jnp.bfloat16), sum_up.astype(jnp.bfloat16), sum_down.astype(jnp.bfloat16))
```

```python
import functools
import math

import jax
import jax.numpy as jnp
from jax import lax
from jax.experimental import pallas as pl
from jax.experimental.pallas import tpu as pltpu
from jax.sharding import PartitionSpec as P

FF = 36864
BLOCK = 128
TILE = 512
LANES = 128
F32 = jnp.float32
BF16 = jnp.bfloat16


def gelu_pair(value):
    scale = 0.7978845608028654
    cubic = 0.044715
    square = value * value
    half = 0.5 + 0.5 * jnp.tanh(value * (scale + scale * cubic * square))
    act = value * half
    slope = half + act * (1.0 - half) * (2.0 * scale + 6.0 * scale * cubic * square)
    return act, slope


def nn(left, right):
    return jnp.dot(left, right, preferred_element_type=F32)


def nt(left, right):
    return lax.dot_general(left, right, (((1,), (1,)), ((), ())), preferred_element_type=F32)


def tile_of(local):
    return TILE if local % TILE == 0 else local // 2 if local % 256 == 0 else local


def whole(shape):
    return pl.BlockSpec(shape, lambda j, *_: (0,) * len(shape), pipeline_mode=pl.Buffered(1))


def params():
    return pltpu.CompilerParams(vmem_limit_bytes=66_000_000, dimension_semantics=("arbitrary",))


def cost(products, rows, features, hidden):
    return pl.CostEstimate(
        flops=2 * products * rows * features * hidden,
        bytes_accessed=6 * features * hidden,
        transcendentals=0,
    )


def own_up_kernel(width_ref, x_ref, wg_ref, wu_ref, hid_ref, act_ref, us_ref):
    rows, tile = x_ref.shape[0], wg_ref.shape[1]
    gate = nn(x_ref[...], wg_ref[...])
    up = nn(x_ref[...], wu_ref[...])
    column = pl.program_id(0) * tile + lax.broadcasted_iota(jnp.int32, (BLOCK, tile), 1)
    for block in range(rows // BLOCK):
        here = slice(block * BLOCK, (block + 1) * BLOCK)
        active = column < width_ref[block]
        act, slope = gelu_pair(gate[here])
        act = jnp.where(active, act, 0.0)
        slope = jnp.where(active, slope, 0.0)
        hid_ref[here, :] = (act * up[here]).astype(BF16)
        act_ref[here, :] = act.astype(BF16)
        us_ref[here, :] = (up[here] * slope).astype(BF16)


def own_up(widths, x, wg, wu):
    rows, features = x.shape
    local = wg.shape[1]
    tile = tile_of(local)
    weight = pl.BlockSpec((features, tile), lambda j, *_: (0, j))
    out = pl.BlockSpec((rows, tile), lambda j, *_: (0, j))
    return pl.pallas_call(
        own_up_kernel,
        grid_spec=pltpu.PrefetchScalarGridSpec(
            num_scalar_prefetch=1,
            grid=(local // tile,),
            in_specs=[whole((rows, features)), weight, weight],
            out_specs=[out] * 3,
        ),
        out_shape=[jax.ShapeDtypeStruct((rows, local), BF16)] * 3,
        compiler_params=params(),
        cost_estimate=cost(2, rows, features, local),
        name="own_up",
    )(widths, x, wg, wu)


def turn_kernel(from_ref, to_ref):
    to_ref[...] = from_ref[...].T


def turn(array):
    return pl.pallas_call(
        turn_kernel,
        out_shape=jax.ShapeDtypeStruct(array.shape[::-1], array.dtype),
        in_specs=[pl.BlockSpec(memory_space=pltpu.VMEM)],
        out_specs=pl.BlockSpec(memory_space=pltpu.VMEM),
        compiler_params=pltpu.CompilerParams(vmem_limit_bytes=32_000_000),
        cost_estimate=pl.CostEstimate(flops=10**9, bytes_accessed=4 * array.size, transcendentals=0),
        name="turn",
    )(array)


def own_back_kernel(dy_ref, wd_ref, hid_ref, act_ref, us_ref, dg_ref, du_ref, out_ref, acc):
    step = pl.program_id(0)

    @pl.when(step == 0)
    def _():
        acc[...] = jnp.zeros_like(acc)

    back = nt(dy_ref[...], wd_ref[...])
    acc[...] += nn(hid_ref[...], wd_ref[...])
    dg_ref[...] = (back * us_ref[...].astype(F32)).astype(BF16)
    du_ref[...] = (back * act_ref[...].astype(F32)).astype(BF16)

    @pl.when(step == pl.num_programs(0) - 1)
    def _():
        out_ref[...] = acc[...].T.astype(BF16)


def own_back(dy, wd, hid, act, us):
    rows, features = dy.shape
    local = wd.shape[0]
    tile = tile_of(local)
    mid = pl.BlockSpec((rows, tile), lambda j: (0, j))
    return pl.pallas_call(
        own_back_kernel,
        grid=(local // tile,),
        in_specs=[whole((rows, features)), pl.BlockSpec((tile, features), lambda j: (j, 0)), mid, mid, mid],
        out_specs=[mid, mid, pl.BlockSpec((features, rows), lambda j: (0, 0))],
        out_shape=[jax.ShapeDtypeStruct((rows, local), BF16)] * 2
        + [jax.ShapeDtypeStruct((features, rows), BF16)],
        scratch_shapes=[pltpu.VMEM((rows, features), F32)],
        compiler_params=params(),
        cost_estimate=cost(2, rows, features, local),
        name="own_back",
    )(dy, wd, hid, act, us)


def own_ig_kernel(wg_ref, wu_ref, dg_ref, du_ref, ig_ref, acc):
    step = pl.program_id(0)

    @pl.when(step == 0)
    def _():
        acc[...] = jnp.zeros_like(acc)

    acc[...] += nt(dg_ref[...], wg_ref[...]) + nt(du_ref[...], wu_ref[...])

    @pl.when(step == pl.num_programs(0) - 1)
    def _():
        ig_ref[...] = acc[...].T.astype(BF16)


def own_ig(wg, wu, dg, du):
    rows, local = dg.shape
    features = wg.shape[0]
    tile = tile_of(local)
    weight = pl.BlockSpec((features, tile), lambda j: (0, j))
    mid = pl.BlockSpec((rows, tile), lambda j: (0, j))
    return pl.pallas_call(
        own_ig_kernel,
        grid=(local // tile,),
        in_specs=[weight, weight, mid, mid],
        out_specs=pl.BlockSpec((features, rows), lambda j: (0, 0)),
        out_shape=jax.ShapeDtypeStruct((features, rows), BF16),
        scratch_shapes=[pltpu.VMEM((rows, features), F32)],
        compiler_params=params(),
        cost_estimate=cost(2, rows, features, local),
        name="own_ig",
    )(wg, wu, dg, du)


def stage(x, dy, wg, wu, wd, width_ref, first, column, hid_ref, dg_ref, du_ref, base):
    gate = nn(x, wg)
    up = nn(x, wu)
    back = nt(dy, wd)
    for block in range(gate.shape[0] // BLOCK):
        here = slice(block * BLOCK, (block + 1) * BLOCK)
        there = slice(base + block * BLOCK, base + (block + 1) * BLOCK)
        active = column < width_ref[first + block]
        act, slope = gelu_pair(gate[here])
        kept = jnp.where(active, back[here], 0.0)
        hid_ref[there, :] = jnp.where(active, act * up[here], 0.0).astype(BF16)
        dg_ref[there, :] = (kept * (up[here] * slope)).astype(BF16)
        du_ref[there, :] = (kept * act).astype(BF16)


def columns(tile):
    return pl.program_id(0) * tile + lax.broadcasted_iota(jnp.int32, (BLOCK, tile), 1)


def near_kernel(width_ref, x_ref, dy_ref, wg_ref, wu_ref, wd_ref, hid_ref, dg_ref, du_ref):
    stage(
        x_ref[...], dy_ref[...], wg_ref[...], wu_ref[...], wd_ref[...],
        width_ref, 0, columns(wg_ref.shape[1]), hid_ref, dg_ref, du_ref, 0,
    )


def near(widths, x, dy, wg, wu, wd):
    rows, features = x.shape
    local = wg.shape[1]
    tile = tile_of(local)
    weight = pl.BlockSpec((features, tile), lambda j, *_: (0, j))
    mid = pl.BlockSpec((rows, tile), lambda j, *_: (0, j))
    return pl.pallas_call(
        near_kernel,
        grid_spec=pltpu.PrefetchScalarGridSpec(
            num_scalar_prefetch=1,
            grid=(local // tile,),
            in_specs=[whole(x.shape), whole(dy.shape), weight, weight, pl.BlockSpec((tile, features), lambda j, *_: (j, 0))],
            out_specs=[mid] * 3,
        ),
        out_shape=[jax.ShapeDtypeStruct((rows, local), BF16)] * 3,
        compiler_params=params(),
        cost_estimate=cost(3, rows, features, local),
        name="near",
    )(widths, x, dy, wg, wu, wd)


def far_kernel(given, groups, width_ref, group_ref, *refs):
    total = given + groups
    xs, dys = refs[:total], refs[total : 2 * total]
    wg_ref, wu_ref, wd_ref = refs[2 * total : 2 * total + 3]
    ready = refs[2 * total + 3 : 2 * total + 3 + 3 * given]
    gg_ref, gu_ref, gd_ref, hid, dg, du, xt, dyt, window = refs[2 * total + 3 + 3 * given :]
    rows = xs[0].shape[0]
    share = xt.shape[0]

    @pl.when(pl.program_id(0) == 0)
    def _():
        offset = group_ref[0] * share
        base = pl.multiple_of(offset // LANES * LANES, LANES)
        lead = pl.multiple_of(offset - base, math.gcd(share, LANES))
        for from_refs, to in ((xs, xt), (dys, dyt)):
            for which, ref in enumerate(from_refs):
                window[...] = ref[:, pl.ds(base, window.shape[0])].T
                to[:, which * rows : (which + 1) * rows] = window[pl.ds(lead, share), :]

    for which in range(given):
        there = slice(which * rows, (which + 1) * rows)
        for to, ref in zip((hid, dg, du), ready[3 * which : 3 * which + 3]):
            to[there, :] = ref[...]
    column = columns(wg_ref.shape[1])
    for group in range(groups):
        stage(
            xs[given + group][...], dys[given + group][...], wg_ref[...], wu_ref[...], wd_ref[...],
            width_ref, group * (rows // BLOCK), column, hid, dg, du, (given + group) * rows,
        )
    gg_ref[...] = nn(xt[...], dg[...]).astype(BF16)
    gu_ref[...] = nn(xt[...], du[...]).astype(BF16)
    gd_ref[...] = nn(dyt[...], hid[...]).astype(BF16)


def far(widths, group, share, xs, dys, wg, wu, wd, ready):
    rows, features = xs[0].shape
    local = wg.shape[1]
    given = len(ready) // 3
    groups = len(xs) - given
    tile = tile_of(local)
    window = min(features, -(-(share + LANES - math.gcd(share, LANES)) // LANES) * LANES)
    weight = pl.BlockSpec((features, tile), lambda j, *_: (0, j))
    mid = pl.BlockSpec((rows, tile), lambda j, *_: (0, j))
    out = pl.BlockSpec((share, tile), lambda j, *_: (0, j))
    return pl.pallas_call(
        functools.partial(far_kernel, given, groups),
        grid_spec=pltpu.PrefetchScalarGridSpec(
            num_scalar_prefetch=2,
            grid=(local // tile,),
            in_specs=[whole(a.shape) for a in (*xs, *dys)]
            + [weight, weight, pl.BlockSpec((tile, features), lambda j, *_: (j, 0))]
            + [mid] * len(ready),
            out_specs=[out] * 3,
            scratch_shapes=[pltpu.VMEM((len(xs) * rows, tile), BF16)] * 3
            + [pltpu.VMEM((share, len(xs) * rows), BF16)] * 2
            + [pltpu.VMEM((window, rows), BF16)],
        ),
        out_shape=[jax.ShapeDtypeStruct((share, local), BF16)] * 3,
        compiler_params=params(),
        cost_estimate=cost(3 * groups + 3, rows, features, local),
        name="far",
    )(widths, group, *xs, *dys, wg, wu, wd, *ready)


def body(tokens, cotangent, prefix, gate_weight, up_weight, down_weight):
    n_dp, n_col = lax.axis_size("dp"), lax.axis_size("col")
    group, col = lax.axis_index("dp"), lax.axis_index("col")
    even = col % 2 == 0
    rows = tokens.shape[0]
    features, local = gate_weight.shape
    share = features // n_dp
    both = ("dp", "col")
    partner = [(c, c ^ 1) for c in range(n_col)]

    def between(even_step, odd_step):
        return [
            (i * n_col + c, (i ^ (odd_step if c % 2 else even_step)) * n_col + c)
            for i in range(n_dp)
            for c in range(n_col)
        ]

    xt = lax.all_gather(tokens.T, "col", axis=0, tiled=True)
    dyt = lax.all_gather(cotangent.T, "col", axis=0, tiled=True)
    widths = jnp.left_shift(jnp.int32(FF // 8), lax.all_gather(prefix, "dp", axis=0)) - col * local
    first = jnp.where(even, 1, 2)
    own_widths = lax.dynamic_index_in_dim(widths, group, 0, keepdims=False)
    near_widths = lax.dynamic_index_in_dim(widths, group ^ first, 0, keepdims=False)
    side_widths = lax.dynamic_index_in_dim(widths, group ^ (3 - first), 0, keepdims=False)
    corner_widths = lax.dynamic_index_in_dim(widths, group ^ 3, 0, keepdims=False)
    far_widths = jnp.concatenate([side_widths, corner_widths])

    x = turn(xt)
    near_x = lax.ppermute(x, both, between(1, 2))
    hid, act, us = own_up(own_widths, x, gate_weight, up_weight)

    dyt, hid = lax.optimization_barrier((dyt, hid))
    dy = turn(dyt)
    near_dy = lax.ppermute(dy, both, between(1, 2))
    side_x = lax.ppermute(near_x, "col", partner)
    dg, du, out = own_back(dy, down_weight, hid, act, us)
    output = lax.psum_scatter(out, "col", scatter_dimension=0, tiled=True).T

    near_x, near_dy, dg = lax.optimization_barrier((near_x, near_dy, dg))
    corner = lax.ppermute(jnp.where(even, near_x, near_dy), both, between(2, 1))
    side_dy = lax.ppermute(near_dy, "col", partner)
    ig = own_ig(gate_weight, up_weight, dg, du)
    input_grad = lax.psum_scatter(ig, "col", scatter_dimension=0, tiled=True).T

    corner, side_x, side_dy, near_x, ig = lax.optimization_barrier((corner, side_x, side_dy, near_x, ig))
    corner_other = lax.ppermute(corner, "col", partner)
    ready = near(near_widths, near_x, near_dy, gate_weight, up_weight, down_weight)

    corner, corner_other, hid = lax.optimization_barrier((corner, corner_other, hid))
    corner_x = jnp.where(even, corner, corner_other)
    corner_dy = jnp.where(even, corner_other, corner)

    gg, gu, gd = far(
        far_widths, group.reshape(1), share, [x, near_x, side_x, corner_x], [dy, near_dy, side_dy, corner_dy],
        gate_weight, up_weight, down_weight, [hid, dg, du, *ready],
    )
    return output, input_grad, gg, gu, gd.T


def solution(mesh):
    return jax.shard_map(
        body,
        mesh=mesh,
        in_specs=(
            P("dp", "col"),
            P("dp", "col"),
            P("dp"),
            P(None, "col"),
            P(None, "col"),
            P("col", None),
        ),
        out_specs=(P("dp", "col"), P("dp", "col"), P("dp", "col"), P("dp", "col"), P("col", "dp")),
        check_vma=False,
    )
```

```python
import functools
import math

import jax
import jax.numpy as jnp
from jax import lax
from jax.experimental import pallas as pl
from jax.experimental.pallas import tpu as pltpu
from jax.sharding import PartitionSpec as P


FF = 36864
BLOCK = 128
TILE = 512
LANES = 128
F32 = jnp.float32
BF16 = jnp.bfloat16


def gelu_pair(value):
    scale = 0.7978845608028654
    cubic = 0.044715
    square = value * value
    half = 0.5 + 0.5 * jnp.tanh(value * (scale + scale * cubic * square))
    act = value * half
    slope = half + act * (1.0 - half) * (2.0 * scale + 6.0 * scale * cubic * square)
    return act, slope


def nn(left, right):
    return jnp.dot(left, right, preferred_element_type=F32)


def nt(left, right):
    return lax.dot_general(left, right, (((1,), (1,)), ((), ())), preferred_element_type=F32)


def tile_of(local):
    return TILE if local % TILE == 0 else local // 2 if local % 256 == 0 else local


def whole(shape):
    return pl.BlockSpec(shape, lambda j, *_: (0,) * len(shape), pipeline_mode=pl.Buffered(1))


def params():
    return pltpu.CompilerParams(vmem_limit_bytes=66_000_000, dimension_semantics=("arbitrary",))


def cost(products, rows, features, hidden):
    return pl.CostEstimate(
        flops=2 * products * rows * features * hidden,
        bytes_accessed=6 * features * hidden,
        transcendentals=0,
    )


def own_up_kernel(width_ref, x_ref, wg_ref, wu_ref, hid_ref, act_ref, us_ref):
    rows, tile = x_ref.shape[0], wg_ref.shape[1]
    gate = nn(x_ref[...], wg_ref[...])
    up = nn(x_ref[...], wu_ref[...])
    column = pl.program_id(0) * tile + lax.broadcasted_iota(jnp.int32, (BLOCK, tile), 1)
    for block in range(rows // BLOCK):
        here = slice(block * BLOCK, (block + 1) * BLOCK)
        active = column < width_ref[block]
        act, slope = gelu_pair(gate[here])
        act = jnp.where(active, act, 0.0)
        slope = jnp.where(active, slope, 0.0)
        hid_ref[here, :] = (act * up[here]).astype(BF16)
        act_ref[here, :] = act.astype(BF16)
        us_ref[here, :] = (up[here] * slope).astype(BF16)


def own_up(widths, x, wg, wu):
    rows, features = x.shape
    local = wg.shape[1]
    tile = tile_of(local)
    weight = pl.BlockSpec((features, tile), lambda j, *_: (0, j))
    out = pl.BlockSpec((rows, tile), lambda j, *_: (0, j))
    return pl.pallas_call(
        own_up_kernel,
        grid_spec=pltpu.PrefetchScalarGridSpec(
            num_scalar_prefetch=1,
            grid=(local // tile,),
            in_specs=[whole((rows, features)), weight, weight],
            out_specs=[out] * 3,
        ),
        out_shape=[jax.ShapeDtypeStruct((rows, local), BF16)] * 3,
        compiler_params=params(),
        cost_estimate=cost(2, rows, features, local),
        name="own_up",
    )(widths, x, wg, wu)


def turn_kernel(from_ref, to_ref):
    to_ref[...] = from_ref[...].T


def turn(array):
    rows, columns = array.shape
    return pl.pallas_call(
        turn_kernel,
        grid=(columns // LANES,),
        in_specs=[pl.BlockSpec((rows, LANES), lambda j: (0, j))],
        out_specs=pl.BlockSpec((LANES, rows), lambda j: (j, 0)),
        out_shape=jax.ShapeDtypeStruct((columns, rows), array.dtype),
        compiler_params=pltpu.CompilerParams(vmem_limit_bytes=16_000_000),
        cost_estimate=pl.CostEstimate(flops=10**9, bytes_accessed=4 * array.size, transcendentals=0),
        name="turn",
    )(array)


def own_down_kernel(
    dy_ref, wg_ref, wu_ref, wd_ref, hid_ref, act_ref, us_ref,
    dg_ref, du_ref, out_ref, ig_ref, acc_out, acc_ig,
):
    step = pl.program_id(0)

    @pl.when(step == 0)
    def _():
        acc_out[...] = jnp.zeros_like(acc_out)
        acc_ig[...] = jnp.zeros_like(acc_ig)

    back = nt(dy_ref[...], wd_ref[...])
    acc_out[...] += nn(hid_ref[...], wd_ref[...])
    dg_ref[...] = (back * us_ref[...].astype(F32)).astype(BF16)
    du_ref[...] = (back * act_ref[...].astype(F32)).astype(BF16)
    acc_ig[...] += nt(dg_ref[...], wg_ref[...]) + nt(du_ref[...], wu_ref[...])

    @pl.when(step == pl.num_programs(0) - 1)
    def _():
        out_ref[...] = acc_out[...].T.astype(BF16)
        ig_ref[...] = acc_ig[...].T.astype(BF16)


def own_down(dy, wg, wu, wd, hid, act, us):
    rows, features = dy.shape
    local = wg.shape[1]
    tile = tile_of(local)
    weight = pl.BlockSpec((features, tile), lambda j: (0, j))
    mid = pl.BlockSpec((rows, tile), lambda j: (0, j))
    end = pl.BlockSpec((features, rows), lambda j: (0, 0))
    return pl.pallas_call(
        own_down_kernel,
        grid=(local // tile,),
        in_specs=[
            whole((rows, features)), weight, weight,
            pl.BlockSpec((tile, features), lambda j: (j, 0)), mid, mid, mid,
        ],
        out_specs=[mid, mid, end, end],
        out_shape=[jax.ShapeDtypeStruct((rows, local), BF16)] * 2
        + [jax.ShapeDtypeStruct((features, rows), BF16)] * 2,
        scratch_shapes=[pltpu.VMEM((rows, features), F32)] * 2,
        compiler_params=params(),
        cost_estimate=cost(4, rows, features, local),
        name="own_down",
    )(dy, wg, wu, wd, hid, act, us)


def stage(x, dy, wg, wu, wd, width_ref, first, column, hid_ref, dg_ref, du_ref, base):
    size = column.shape[0]
    gate = nn(x, wg)
    up = nn(x, wu)
    back = nt(dy, wd)
    for block in range(gate.shape[0] // size):
        here = slice(block * size, (block + 1) * size)
        there = slice(base + block * size, base + (block + 1) * size)
        active = column < width_ref[first + block]
        act, slope = gelu_pair(gate[here])
        kept = jnp.where(active, back[here], 0.0)
        hid_ref[there, :] = jnp.where(active, act * up[here], 0.0).astype(BF16)
        dg_ref[there, :] = (kept * (up[here] * slope)).astype(BF16)
        du_ref[there, :] = (kept * act).astype(BF16)


def columns(size, tile):
    return pl.program_id(0) * tile + lax.broadcasted_iota(jnp.int32, (size, tile), 1)


def near_kernel(width_ref, x_ref, dy_ref, wg_ref, wu_ref, wd_ref, hid_ref, dg_ref, du_ref):
    stage(
        x_ref[...], dy_ref[...], wg_ref[...], wu_ref[...], wd_ref[...],
        width_ref, 0, columns(BLOCK, wg_ref.shape[1]), hid_ref, dg_ref, du_ref, 0,
    )


def near(widths, x, dy, wg, wu, wd):
    rows, features = x.shape
    local = wg.shape[1]
    tile = tile_of(local)
    weight = pl.BlockSpec((features, tile), lambda j, *_: (0, j))
    mid = pl.BlockSpec((rows, tile), lambda j, *_: (0, j))
    return pl.pallas_call(
        near_kernel,
        grid_spec=pltpu.PrefetchScalarGridSpec(
            num_scalar_prefetch=1,
            grid=(local // tile,),
            in_specs=[whole(x.shape), whole(dy.shape), weight, weight, pl.BlockSpec((tile, features), lambda j, *_: (j, 0))],
            out_specs=[mid] * 3,
        ),
        out_shape=[jax.ShapeDtypeStruct((rows, local), BF16)] * 3,
        compiler_params=params(),
        cost_estimate=cost(3, rows, features, local),
        name="near",
    )(widths, x, dy, wg, wu, wd)


def far_kernel(given, width_ref, place_ref, *refs):
    (
        own_x, near_x, side_x, part_x, rest_x, own_dy, near_dy, side_dy, part_dy, rest_dy,
        wg_ref, wu_ref, wd_ref,
    ) = refs[:13]
    ready = refs[13 : 13 + 3 * given]
    gg_ref, gu_ref, gd_ref, hid, dg, du, xt, dyt, window, corner_x, corner_dy = refs[13 + 3 * given :]
    rows = own_x.shape[0]
    share = xt.shape[0]
    half = rows // 2

    @pl.when(pl.program_id(0) == 0)
    def _():
        mine = pl.multiple_of(place_ref[1] * half, half)
        others = pl.multiple_of(half - place_ref[1] * half, half)
        corner_x[pl.ds(mine, half), :] = part_x[...]
        corner_x[pl.ds(others, half), :] = rest_x[...]
        corner_dy[pl.ds(mine, half), :] = part_dy[...]
        corner_dy[pl.ds(others, half), :] = rest_dy[...]
        offset = place_ref[0] * share
        base = pl.multiple_of(offset // LANES * LANES, LANES)
        lead = pl.multiple_of(offset - base, math.gcd(share, LANES))
        for from_refs, to in (
            ((own_x, near_x, side_x, corner_x), xt),
            ((own_dy, near_dy, side_dy, corner_dy), dyt),
        ):
            for which, ref in enumerate(from_refs):
                window[...] = ref[:, pl.ds(base, window.shape[0])].T
                to[:, which * rows : (which + 1) * rows] = window[pl.ds(lead, share), :]

    for which in range(given):
        there = slice(which * rows, (which + 1) * rows)
        for to, ref in zip((hid, dg, du), ready[3 * which : 3 * which + 3]):
            to[there, :] = ref[...]
    column = columns(BLOCK, wg_ref.shape[1])
    for which, (x, dy) in enumerate(((side_x, side_dy), (corner_x, corner_dy))):
        stage(
            x[...], dy[...], wg_ref[...], wu_ref[...], wd_ref[...],
            width_ref, which * (rows // BLOCK), column, hid, dg, du, (given + which) * rows,
        )
    gg_ref[...] = nn(xt[...], dg[...]).astype(BF16)
    gu_ref[...] = nn(xt[...], du[...]).astype(BF16)
    gd_ref[...] = nn(dyt[...], hid[...]).astype(BF16)


def far(widths, place, share, xs, dys, wg, wu, wd, ready):
    rows, features = xs[0].shape
    local = wg.shape[1]
    given = len(ready) // 3
    tokens = (given + 2) * rows
    tile = tile_of(local)
    window = min(features, -(-(share + LANES - math.gcd(share, LANES)) // LANES) * LANES)
    weight = pl.BlockSpec((features, tile), lambda j, *_: (0, j))
    mid = pl.BlockSpec((rows, tile), lambda j, *_: (0, j))
    out = pl.BlockSpec((share, tile), lambda j, *_: (0, j))
    return pl.pallas_call(
        functools.partial(far_kernel, given),
        grid_spec=pltpu.PrefetchScalarGridSpec(
            num_scalar_prefetch=2,
            grid=(local // tile,),
            in_specs=[whole(a.shape) for a in (*xs, *dys)]
            + [weight, weight, pl.BlockSpec((tile, features), lambda j, *_: (j, 0))]
            + [mid] * len(ready),
            out_specs=[out] * 3,
            scratch_shapes=[pltpu.VMEM((tokens, tile), BF16)] * 3
            + [pltpu.VMEM((share, tokens), BF16)] * 2
            + [pltpu.VMEM((window, rows), BF16)]
            + [pltpu.VMEM((rows, features), BF16)] * 2,
        ),
        out_shape=[jax.ShapeDtypeStruct((share, local), BF16)] * 3,
        compiler_params=params(),
        cost_estimate=cost(9, rows, features, local),
        name="far",
    )(widths, place, *xs, *dys, wg, wu, wd, *ready)


def body(tokens, cotangent, prefix, gate_weight, up_weight, down_weight):
    n_dp, n_col = lax.axis_size("dp"), lax.axis_size("col")
    group, col = lax.axis_index("dp"), lax.axis_index("col")
    even = col % 2 == 0
    rows = tokens.shape[0]
    features, local = gate_weight.shape
    share = features // n_dp
    both = ("dp", "col")
    partner = [(c, c ^ 1) for c in range(n_col)]

    def between(even_step, odd_step):
        return [
            (i * n_col + c, (i ^ (odd_step if c % 2 else even_step)) * n_col + c)
            for i in range(n_dp)
            for c in range(n_col)
        ]

    xt = lax.all_gather(tokens.T, "col", axis=0, tiled=True)
    dyt = lax.all_gather(cotangent.T, "col", axis=0, tiled=True)
    widths = jnp.left_shift(jnp.int32(FF // 8), lax.all_gather(prefix, "dp", axis=0)) - col * local
    first = jnp.where(even, 1, 2)
    own_widths = lax.dynamic_index_in_dim(widths, group, 0, keepdims=False)
    near_widths = lax.dynamic_index_in_dim(widths, group ^ first, 0, keepdims=False)
    side_widths = lax.dynamic_index_in_dim(widths, group ^ (3 - first), 0, keepdims=False)
    corner_widths = lax.dynamic_index_in_dim(widths, group ^ 3, 0, keepdims=False)
    far_widths = jnp.concatenate([side_widths, corner_widths])

    half = rows // 2
    odd = col % 2

    def send(array):
        part = lax.dynamic_slice(array, (odd * half, 0), (half, features))
        whole_one = lax.ppermute(array, both, between(1, 2))
        half_one = lax.ppermute(part, both, between(3, 3))
        return whole_one, half_one

    x = turn(xt)
    near_x, part_x = send(x)
    hid, act, us = own_up(own_widths, x, gate_weight, up_weight)

    dyt, hid = lax.optimization_barrier((dyt, hid))
    dy = turn(dyt)
    near_dy, part_dy = send(dy)
    dg, du, out, ig = own_down(dy, gate_weight, up_weight, down_weight, hid, act, us)
    output = lax.psum_scatter(out, "col", scatter_dimension=0, tiled=True).T
    input_grad = lax.psum_scatter(ig, "col", scatter_dimension=0, tiled=True).T

    near_x, part_x, near_dy, part_dy, dg = lax.optimization_barrier((near_x, part_x, near_dy, part_dy, dg))
    side_x, rest_x, side_dy, rest_dy = [
        lax.ppermute(a, "col", partner) for a in (near_x, part_x, near_dy, part_dy)
    ]
    ready = near(near_widths, near_x, near_dy, gate_weight, up_weight, down_weight)
    gg, gu, gd = far(
        far_widths, jnp.stack([group, odd]), share,
        [x, near_x, side_x, part_x, rest_x], [dy, near_dy, side_dy, part_dy, rest_dy],
        gate_weight, up_weight, down_weight, [hid, dg, du, *ready],
    )
    return output, input_grad, gg, gu, gd.T


def solution(mesh):
    return jax.shard_map(
        body,
        mesh=mesh,
        in_specs=(
            P("dp", "col"),
            P("dp", "col"),
            P("dp"),
            P(None, "col"),
            P(None, "col"),
            P("col", None),
        ),
        out_specs=(P("dp", "col"), P("dp", "col"), P("dp", "col"), P("dp", "col"), P("col", "dp")),
        check_vma=False,
    )
```
